32 devices in a mesh: depth: 2 (over x), lat: 16 (over z, y, core).
Axes of the slice: x: 2, y: 2, z: 4, core: 2. Of those that a mesh axis runs over, the one named last changes fastest.
Arguments:
- displacement: float32 [3, 16, 128, 256], P(None, 'depth', 'lat'), may hold values from -6 to 6
- velocity: float32 [3, 16, 128, 256], P(None, 'depth', 'lat'), may hold values from -6 to 6
- inverse_mass: float32 [16, 128, 256], P('depth', 'lat'), may hold values from 0.5 to 2
- material: int32 [16, 128, 256], P('depth', 'lat'), may hold values from 0 to 7
- dilation_table: float32 [8], replicated, may hold values from 0.5 to 2
- shear_table: float32 [8], replicated, may hold values from 0.5 to 2
- stiffness_pair: float32 [2, 24, 24], replicated, may hold values from -1.5 to 3.5, as said below
- impedance: float32 [3], replicated, may hold values from 0.5 to 2
- bedrock_mask: int32 [128, 256], P('lat'), may hold values 0 or 1
- incident: float32 [6, 3, 128, 256], P(None, None, 'lat'), may hold values from -6 to 6
Outputs:
- new_displacement: float32 [3, 16, 128, 256], P(None, 'depth', 'lat')
- new_velocity: float32 [3, 16, 128, 256], P(None, 'depth', 'lat')
The draws below stay inside these ranges and needn't reach their ends.
Inputs may be any that keep to these rules, and one draw needn't show every extreme that they name: `stiffness_pair`: symmetric positive definite.
All inputs are finite; a program needn't handle non-finite values. No bound on the sum of `bedrock_mask` on one device may be relied on, other than what follows from the above.
Results may differ from the reference program's by a relative error of at most 0.00016.
Values sent between devices are 32-bit elements; how exact they have to be, the bound alone decides.
A program may use at most 64 MiB of HBM per device.

```python
import math
import jax
import jax.numpy as jnp
from jax import lax

NXC = 256
STEPS = 6
NMAT = 8
NZ = 16
NY = 128


def draw_stiffness_pair(key, part):
    factor = jax.random.normal(key, (2, 24, 24), jnp.float32)
    square = jnp.einsum('aij,akj->aik', factor, factor) / 48.0
    return 0.5 * jnp.eye(24, dtype=jnp.float32)[None] + square


def touch_ends(result, stream_key, low, top_value):
    longest = result.shape.index(max(result.shape))
    spots = []
    for shift in (0, 1):
        where = [jax.random.randint(jax.random.fold_in(stream_key, axis), (), 0, length) for axis, length in enumerate(result.shape)]
        where[longest] = (where[longest] + shift) % result.shape[longest]
        spots.append(tuple(where))
    return result.at[spots[0]].set(low).at[spots[1]].set(top_value)


def block_levels(key, dims, shards, least, high):
    def one(dim, shards_of):
        heights = jax.random.uniform(jax.random.fold_in(jax.random.fold_in(key, 6), dim), (shards_of,), jnp.float32, least / len(shards), high / len(shards))
        return jnp.repeat(jnp.exp(heights), dims[dim] // shards_of).reshape((-1,) + (1,) * (len(dims) - dim - 1))

    loudness = one(*shards[0])
    for cut in shards[1:]:
        loudness = loudness * one(*cut)
    return loudness


def noise(own_key, dims, width, most, shards=(), held_as=jnp.bfloat16):
    drawn = jax.random.normal(own_key, dims, jnp.float32) * width
    if len(shards) > 0:
        drawn = block_levels(own_key, dims, shards, -0.22, 0.18) * drawn
    return jnp.clip(drawn, min=-most, max=most).astype(held_as)


def setup_inputs(seed: int = 0) -> dict:
    key_of = jax.random.split(jax.random.key(seed), 11)
    return {
        "displacement": noise(key_of[0], (3, NZ, NY, NXC), 1.0, 6.0, ((1, 2), (2, 16)), jnp.float32),
        "velocity": noise(key_of[1], (3, NZ, NY, NXC), 1.0, 6.0, ((1, 2), (2, 16)), jnp.float32),
        "inverse_mass": jnp.clip(jnp.exp(math.log(2.0) - 1.3862944 * jax.random.uniform(key_of[2], (NZ, NY, NXC), jnp.float32) ** block_levels(key_of[2], (NZ, NY, NXC), ((0, 2), (1, 16)), -0.2, 0.2)), 0.5, 2.0),
        "material": touch_ends(jax.random.randint(key_of[3], (NZ, NY, NXC), 0, NMAT), jax.random.fold_in(key_of[3], 1), 0, NMAT - 1).astype(jnp.int32),
        "dilation_table": jnp.clip(jnp.exp(jax.random.uniform(key_of[4], (NMAT,), jnp.float32, math.log(0.5), math.log(2.0))), 0.5, 2.0),
        "shear_table": jnp.clip(jnp.exp(jax.random.uniform(key_of[5], (NMAT,), jnp.float32, math.log(0.5), math.log(2.0))), 0.5, 2.0),
        "stiffness_pair": draw_stiffness_pair(jax.random.fold_in(key_of[10], 71), 0),
        "impedance": jnp.clip(jnp.exp(jax.random.uniform(key_of[7], (3,), jnp.float32, math.log(0.5), math.log(2.0))), 0.5, 2.0),
        "bedrock_mask": touch_ends((jax.random.randint(key_of[8], (NY, NXC), 0, 2) < 1).astype(jnp.int32), jax.random.fold_in(key_of[8], 1), 0, 1),
        "incident": noise(key_of[9], (STEPS, 3, NY, NXC), 1.0, 6.0, ((2, 16),), jnp.float32),
    }


time_step = 0.1
highest = lax.Precision.HIGHEST


def layer_forces(lower_plane, upper_plane, dilation_layer, shear_layer, stiffness_rows):
    rows_y, cells_x = dilation_layer.shape
    corners = []
    for node_plane in (lower_plane, upper_plane):
        for shift_y in (0, 1):
            for shift_x in (0, 1):
                corners.append(node_plane[:, shift_y:shift_y + rows_y, shift_x:shift_x + cells_x])
    values = jnp.stack(corners).reshape(24, rows_y * cells_x)
    products = jnp.dot(stiffness_rows, values, precision=highest).reshape(2, 8, 3, rows_y, cells_x)
    element_force = dilation_layer * products[0] + shear_layer * products[1]
    sides = [jnp.zeros((3, rows_y + 1, cells_x + 1), jnp.float32), jnp.zeros((3, rows_y + 1, cells_x + 1), jnp.float32)]
    corner = 0
    for side in range(2):
        for shift_y in (0, 1):
            for shift_x in (0, 1):
                contribution = jnp.pad(element_force[corner], ((0, 0), (shift_y, 1 - shift_y), (shift_x, 1 - shift_x)))
                sides[side] = sides[side] + contribution
                corner += 1
    return sides[0], sides[1]


def assemble(displacement, dilation_field, shear_field, stiffness_rows):
    padded = jnp.pad(displacement, ((0, 0), (0, 1), (0, 1), (0, 1)))
    planes = jnp.moveaxis(padded, 1, 0)

    def advance(carried, inputs):
        lower_plane, upper_plane, dilation_layer, shear_layer = inputs
        low_part, high_part = layer_forces(lower_plane, upper_plane, dilation_layer, shear_layer, stiffness_rows)
        return high_part, carried + low_part

    initial = jnp.zeros(planes.shape[1:], jnp.float32)
    unused, layers = lax.scan(advance, initial, (planes[:-1], planes[1:], dilation_field, shear_field))
    return jnp.moveaxis(layers, 0, 1)[:, :, :-1, :-1]


def reference(displacement, velocity, inverse_mass, material, dilation_table, shear_table, stiffness_pair, impedance, bedrock_mask, incident):
    dilation_field = dilation_table[material]
    shear_field = shear_table[material]
    stiffness_rows = stiffness_pair.reshape(48, 24)
    mask_value = bedrock_mask.astype(jnp.float32)
    bottom = NZ - 1
    for instant in range(STEPS):
        forces = assemble(displacement, dilation_field, shear_field, stiffness_rows)
        traction = impedance[:, None, None] * (2.0 * mask_value * incident[instant] - velocity[:, bottom])
        net_force = (-forces).at[:, bottom].add(traction)
        velocity = velocity + time_step * inverse_mass[None] * net_force
        displacement = displacement + time_step * velocity
    return displacement, velocity
```

```python
import functools

import jax
import jax.numpy as jnp
from jax import lax
from jax.experimental import pallas as pl
from jax.experimental.pallas import tpu as pltpu
from jax.sharding import PartitionSpec as P

time_step = 0.1
WIDTH = 2
f32 = jnp.float32
bf16 = jnp.bfloat16


def kernel(
    cfg, dil_tab, shr_tab, imp_ref, disp, vel, inv, mat, stiff, mask, inc, out_d, out_v,
    tiles, split, moduli, carry, pull, land_y, land_z, land_c, big_s,
    send_sem, recv_sem, q_send, q_recv,
):
    nz, ny, nx, steps, depths, lats, w = cfg
    h = w
    nh = nx // 128
    ext_z = nz + 2 * h
    ext_y = tiles.shape[2] // 8
    nmat = dil_tab.shape[0]
    di = lax.axis_index("depth")
    li = lax.axis_index("lat")
    exists = {}
    for dz in (-1, 0, 1):
        for dy in (-1, 0, 1):
            if dz == 0 and dy == 0:
                continue
            if (dz != 0 and depths == 1) or (dy != 0 and lats == 1):
                continue
            exists[(dz, dy)] = (
                (di + dz >= 0) & (di + dz < depths) & (li + dy >= 0) & (li + dy < lats)
            )
    dirs = list(exists)
    is_bottom = di == depths - 1
    extra = [w - 1 - s % w for s in range(steps)]
    if steps % w:
        for s in range(steps - steps % w, steps):
            extra[s] = steps - 1 - s
    wide = [s for s in range(steps) if extra[s] > 0]
    order = wide + [s for s in range(steps) if extra[s] == 0]
    q_of = {s: i for i, s in enumerate(order)}

    pull[...] = jnp.zeros_like(pull)
    barrier = pltpu.get_barrier_semaphore()
    for dz, dy in dirs:
        @pl.when(exists[(dz, dy)])
        def _(dz=dz, dy=dy):
            pl.semaphore_signal(
                barrier, inc=1, device_id={"depth": di + dz, "lat": li + dy},
                device_id_type=pl.DeviceIdType.MESH,
            )

    def zero_layer(z, c):
        tiles[z] = jnp.zeros(tiles.shape[1:], f32)
        split[z] = jnp.zeros(split.shape[1:], bf16)
        return c

    lax.fori_loop(0, ext_z, zero_layer, 0)

    def fill_layer(z, c):
        for hf in range(nh):
            lanes = slice(hf * 128, hf * 128 + 128)
            for comp in range(3):
                tiles[h + z, hf, pl.ds(h * 8 + comp, ny, stride=8), :] = disp[comp, z, :, lanes]
                tiles[h + z, hf, pl.ds(h * 8 + 3 + comp, ny, stride=8), :] = vel[comp, z, :, lanes]
            tiles[h + z, hf, pl.ds(h * 8 + 6, ny, stride=8), :] = inv[z, :, lanes] * (-time_step)
            tiles[h + z, hf, pl.ds(h * 8 + 7, ny, stride=8), :] = (mat[z, :, lanes] + 1).astype(f32)
        return c

    lax.fori_loop(0, nz, fill_layer, 0)

    @pl.when(is_bottom)
    def _():
        for hf in range(nh):
            lanes = slice(hf * 128, hf * 128 + 128)
            twice = 2.0 * mask[:, lanes].astype(f32)
            for s in range(steps):
                for comp in range(3):
                    pull[q_of[s], hf, pl.ds(h * 8 + 3 + comp, ny, stride=8), :] = (
                        imp_ref[comp] * (twice * inc[s, comp, :, lanes])
                    )

    pl.semaphore_wait(barrier, sum(jnp.where(here, 1, 0) for here in exists.values()))

    def piece(n, dz, dy):
        zs = pl.ds({-1: h, 0: h, 1: h + nz - w}[dz], nz if dz == 0 else w)
        ys = pl.ds({-1: h, 0: h, 1: h + ny - w}[dy] * 8, (ny if dy == 0 else w) * 8)
        if dz == 0:
            dst = land_y.at[n, (1 - dy) // 2]
        elif dy == 0:
            dst = land_z.at[n, (1 - dz) // 2]
        else:
            dst = land_c.at[n, (1 - dz) // 2 * 2 + (1 - dy) // 2]
        k = dirs.index((dz, dy))
        back = dirs.index((-dz, -dy))
        return pltpu.make_async_remote_copy(
            src_ref=tiles.at[zs, :, ys, :],
            dst_ref=dst,
            send_sem=send_sem.at[n, k],
            recv_sem=recv_sem.at[n, back],
            device_id={"depth": di + dz, "lat": li + dy},
            device_id_type=pl.DeviceIdType.MESH,
        )

    def arrived(n, dz, dy):
        if dz == 0:
            dst = land_y.at[n, (1 + dy) // 2]
        elif dy == 0:
            dst = land_z.at[n, (1 + dz) // 2]
        else:
            dst = land_c.at[n, (1 + dz) // 2 * 2 + (1 + dy) // 2]
        k = dirs.index((dz, dy))
        return dst, pltpu.make_async_remote_copy(
            src_ref=dst, dst_ref=dst, send_sem=send_sem.at[n, k], recv_sem=recv_sem.at[n, k],
            device_id={"depth": di + dz, "lat": li + dy},
            device_id_type=pl.DeviceIdType.MESH,
        )

    def pull_copy(dy, waits=False):
        src = pl.ds((h if dy < 0 else h + ny - (w - 1)) * 8, (w - 1) * 8)
        dst = pl.ds((h + ny if dy < 0 else h - (w - 1)) * 8, (w - 1) * 8)
        side = (1 + dy) // 2
        return pltpu.make_async_remote_copy(
            src_ref=pull.at[pl.ds(0, len(wide)), :, src, :],
            dst_ref=pull.at[pl.ds(0, len(wide)), :, dst, :],
            send_sem=q_send.at[side],
            recv_sem=q_recv.at[side if waits else 1 - side],
            device_id={"depth": di, "lat": li + dy},
            device_id_type=pl.DeviceIdType.MESH,
        )

    pull_dirs = [dy for dy in (-1, 1) if w > 1 and (0, dy) in exists]

    def start_all(n):
        for dz, dy in sorted(dirs, key=lambda d: -abs(d[0]) - abs(d[1])):
            @pl.when(exists[(dz, dy)])
            def _(dz=dz, dy=dy):
                piece(n, dz, dy).start()

    rows = lax.broadcasted_iota(jnp.int32, (8, nx), 0)
    columns = lax.broadcasted_iota(jnp.int32, (8, nx), 1)
    top3 = rows < 3
    mid3 = (rows >= 3) & (rows < 6)
    last = columns == nx - 1
    first_column = columns == 0
    keep_in = jnp.where(last, 0.0, 1.0)
    keep_out = jnp.where(first_column, 0.0, 1.0)

    def load_tile(z, y):
        return jnp.concatenate([tiles[z, hf, pl.ds(y * 8, 8), :] for hf in range(nh)], 1)

    def put_split(z, y, tile):
        beside = pltpu.roll(pltpu.roll(tile, nx - 1, 1), 3, 0) * keep_in
        both = jnp.where(top3, tile, beside)
        high = both.astype(bf16).astype(f32)
        split[z, y] = jnp.concatenate([high, both - high], 0).astype(bf16)

    def receive(n, dz, dy):
        @pl.when(exists[(dz, dy)])
        def _():
            ref, copy = arrived(n, dz, dy)
            copy.wait_recv()
            z0 = {-1: 0, 0: h, 1: h + nz}[dz]
            y0 = {-1: 0, 0: h, 1: h + ny}[dy]
            yn = ny if dy == 0 else w

            def body(z, c):
                for y in range(yn):
                    parts = [ref[z, hf, pl.ds(y * 8, 8), :] for hf in range(nh)]
                    for hf in range(nh):
                        tiles[z0 + z, hf, pl.ds((y0 + y) * 8, 8), :] = parts[hf]
                    put_split(z0 + z, y0 + y, jnp.concatenate(parts, 1))
                return c

            lax.fori_loop(0, nz if dz == 0 else w, body, 0)

    def sent(n):
        for dz, dy in dirs:
            @pl.when(exists[(dz, dy)])
            def _(dz=dz, dy=dy):
                piece(n, dz, dy).wait_send()

    def layer(z, e, s, opening):
        ya, yb = h - 1 - e, h + ny - 1 + e
        if not opening:
            @pl.when(is_bottom & (z == h + nz - 1))
            def _():
                wet = jnp.where(rows == 3, imp_ref[0], jnp.where(rows == 4, imp_ref[1], imp_ref[2]))
                for y in range(ya + 1, yb + 1):
                    pulled = jnp.concatenate(
                        [pull[q_of[s], hf, pl.ds(y * 8, 8), :] for hf in range(nh)], 1
                    )
                    carry[y] += jnp.where(mid3, wet * load_tile(z, y) - pulled, 0.0)

        matrix = big_s[...]
        prev_low = prev_high = None
        for y in range(ya, yb + 1):
            values = jnp.concatenate(
                [split[z, y], split[z, y + 1], split[z + 1, y], split[z + 1, y + 1]], 0
            )
            values = jnp.concatenate([values, values], 0)
            product = jnp.dot(matrix, values, preferred_element_type=f32)
            dil = jnp.concatenate([moduli[0, z, hf, pl.ds(y, 1), :] for hf in range(nh)], 1)
            shr = jnp.concatenate([moduli[1, z, hf, pl.ds(y, 1), :] for hf in range(nh)], 1)
            g = dil * product[0:32] + shr * product[32:64]
            if y > ya:
                high = g[16:24] + prev_high
                if not opening:
                    force = (g[0:8] + prev_low) + carry[y]
                    side = pltpu.roll(pltpu.roll(force, 1, 1), 3, 0) * keep_out
                    tile = load_tile(z, y)
                    mass = jnp.concatenate(
                        [tiles[z, hf, pl.ds(y * 8 + 6, 1), :] for hf in range(nh)], 1
                    )
                    moved = tile + jnp.where(mid3, mass * (force + side), 0.0)
                    tile = moved + jnp.where(top3, time_step * pltpu.roll(moved, 5, 0), 0.0)
                    for hf in range(nh):
                        tiles[z, hf, pl.ds(y * 8, 8), :] = tile[:, hf * 128 : hf * 128 + 128]
                    if s < steps - 1:
                        put_split(z, y, tile)
                carry[y] = high
            prev_low, prev_high = g[8:16], g[24:32]

    start_all(0)
    for dy in pull_dirs:
        @pl.when(exists[(0, dy)] & is_bottom)
        def _(dy=dy):
            pull_copy(dy).start()

    i32 = jnp.int32
    ri = lax.broadcasted_iota(i32, (32, 24), 0)
    rc = lax.broadcasted_iota(i32, (32, 24), 1)
    r8 = ri % 8
    left = (r8 < 6) & (rc == (ri // 8) * 6 + jnp.where(r8 < 3, r8 + 3, r8 - 3))
    left = jnp.where(left, 1.0, 0.0).astype(bf16)
    ci = lax.broadcasted_iota(i32, (24, 64), 0)
    cc = lax.broadcasted_iota(i32, (24, 64), 1)
    right = (cc % 8 < 6) & (ci == (cc // 16) * 6 + cc % 8)
    right = jnp.where(right, 1.0, 0.0).astype(bf16)
    blocks = []
    for m in range(2):
        whole = stiff[m]
        upper = whole.astype(bf16)
        lower = (whole - upper.astype(f32)).astype(bf16)
        parts = []
        for part in (upper, lower):
            picked = jnp.dot(left, part, preferred_element_type=f32).astype(bf16)
            parts.append(jnp.dot(picked, right, preferred_element_type=f32))
        blocks.append(jnp.concatenate(parts, 1))
    big_s[...] = jnp.concatenate(blocks, 0).astype(bf16)

    def split_layer(z, c):
        for y in range(ny):
            put_split(h + z, h + y, load_tile(h + z, h + y))
        return c

    lax.fori_loop(0, nz, split_layer, 0)

    def lookup(z, c):
        for hf in range(nh):
            for y0 in range(0, ext_y, 8):
                kind = tiles[z, hf, pl.ds(y0 * 8 + 7, 8, stride=8), :]
                dil = jnp.zeros((8, 128), f32)
                shr = jnp.zeros((8, 128), f32)
                for m in range(nmat):
                    hit = kind == float(m + 1)
                    dil = jnp.where(hit, dil_tab[m], dil)
                    shr = jnp.where(hit, shr_tab[m], shr)
                moduli[0, z, hf, pl.ds(y0, 8), :] = dil
                moduli[1, z, hf, pl.ds(y0, 8), :] = shr
        return c

    for s in range(steps):
        n, e = s // w, extra[s]
        if s % w == 0:
            if s > 0:
                start_all(n)
            for dz, dy in dirs:
                receive(n, dz, dy)
            sent(n)
            if s == 0:
                for dy in pull_dirs:
                    @pl.when(exists[(0, dy)] & is_bottom)
                    def _(dy=dy):
                        pull_copy(dy).wait_send()
                        pull_copy(dy, True).wait_recv()
                lax.fori_loop(0, ext_z, lookup, 0)
        if depths == 1:
            start, count = h, nz
        elif depths == 2:
            start, count = jnp.where(di == 0, h, h - e), nz + e
        else:
            start, count = h - e, nz + 2 * e
        layer(start - 1, e, s, True)

        def body(z, c, start=start, e=e, s=s):
            layer(start + z, e, s, False)
            return c

        lax.fori_loop(0, count, body, 0)

    def give(z, c):
        for hf in range(nh):
            lanes = slice(hf * 128, hf * 128 + 128)
            for comp in range(3):
                out_d[comp, z, :, lanes] = tiles[h + z, hf, pl.ds(h * 8 + comp, ny, stride=8), :]
                out_v[comp, z, :, lanes] = tiles[h + z, hf, pl.ds(h * 8 + 3 + comp, ny, stride=8), :]
        return c

    lax.fori_loop(0, nz, give, 0)


def solution(mesh):
    depths, lats = mesh.shape["depth"], mesh.shape["lat"]

    def per_device(disp, vel, inv, mat, dil_tab, shr_tab, stiff, imp, mask, inc):
        _, nz, ny, nx = disp.shape
        steps = inc.shape[0]
        w = min(WIDTH, nz, ny, steps)
        nh = nx // 128
        groups = -(-steps // w)
        ext_z = nz + 2 * w
        ext_y = -(-(ny + 2 * w) // 8) * 8
        ndirs = (3 if depths > 1 else 1) * (3 if lats > 1 else 1) - 1
        smem = pl.BlockSpec(memory_space=pltpu.SMEM)
        vmem = pl.BlockSpec(memory_space=pltpu.VMEM)
        shape = jax.ShapeDtypeStruct(disp.shape, f32)
        return pl.pallas_call(
            functools.partial(kernel, (nz, ny, nx, steps, depths, lats, w)),
            out_shape=(shape, shape),
            in_specs=[smem] * 3 + [vmem] * 7,
            out_specs=(vmem, vmem),
            scratch_shapes=[
                pltpu.VMEM((ext_z, nh, ext_y * 8, 128), f32),
                pltpu.VMEM((ext_z, ext_y, 16, nx), bf16),
                pltpu.VMEM((2, ext_z, nh, ext_y, 128), f32),
                pltpu.VMEM((ext_y, 8, nx), f32),
                pltpu.VMEM((steps, nh, ext_y * 8, 128), f32),
                pltpu.VMEM((groups, 2, nz, nh, w * 8, 128), f32),
                pltpu.VMEM((groups, 2, w, nh, ny * 8, 128), f32),
                pltpu.VMEM((groups, 4, w, nh, w * 8, 128), f32),
                pltpu.VMEM((64, 128), bf16),
                pltpu.SemaphoreType.DMA((groups, ndirs)),
                pltpu.SemaphoreType.DMA((groups, ndirs)),
                pltpu.SemaphoreType.DMA((2,)),
                pltpu.SemaphoreType.DMA((2,)),
            ],
            compiler_params=pltpu.CompilerParams(
                collective_id=0, has_side_effects=True, vmem_limit_bytes=56 * 1024 * 1024
            ),
        )(dil_tab, shr_tab, imp, disp, vel, inv, mat, stiff, mask, inc)

    field = P(None, "depth", "lat", None)
    node = P("depth", "lat", None)
    in_specs = (field, field, node, node, P(), P(), P(), P(), P("lat", None), P(None, None, "lat", None))
    return jax.shard_map(
        per_device, mesh=mesh, in_specs=in_specs, out_specs=(field, field), check_vma=False
    )
```

```python
import functools

import jax
import jax.numpy as jnp
from jax import lax
from jax.experimental import pallas as pl
from jax.experimental.pallas import tpu as pltpu
from jax.sharding import PartitionSpec as P

time_step = 0.1
WIDTH = 2
f32 = jnp.float32
bf16 = jnp.bfloat16


def kernel(
    cfg, dil_tab, shr_tab, imp_ref, disp, vel, inv, mat, stiff, mask, inc, out_d, out_v,
    grid5, split, moduli, carry, held, pull, land_y, land_z, land_c, big_s,
    send_sem, recv_sem, q_send, q_recv,
):
    nz, ny, nx, steps, depths, lats, w = cfg
    h = w
    nh = nx // 128
    hy = -(-h // 8) * 8
    ext_z = nz + 2 * h
    ext_y = grid5.shape[2]
    tiles = grid5.reshape(ext_z, nh, ext_y * 8, 128)
    nmat = dil_tab.shape[0]
    di = lax.axis_index("depth")
    li = lax.axis_index("lat")
    exists = {}
    for dz in (-1, 0, 1):
        for dy in (-1, 0, 1):
            if dz == 0 and dy == 0:
                continue
            if (dz != 0 and depths == 1) or (dy != 0 and lats == 1):
                continue
            exists[(dz, dy)] = (
                (di + dz >= 0) & (di + dz < depths) & (li + dy >= 0) & (li + dy < lats)
            )
    dirs = list(exists)
    is_bottom = di == depths - 1
    extra = [w - 1 - s % w for s in range(steps)]
    if steps % w:
        for s in range(steps - steps % w, steps):
            extra[s] = steps - 1 - s
    wide = [s for s in range(steps) if extra[s] > 0]
    order = wide + [s for s in range(steps) if extra[s] == 0]
    q_of = {s: i for i, s in enumerate(order)}

    pull[...] = jnp.zeros_like(pull)
    barrier = pltpu.get_barrier_semaphore()
    for dz, dy in dirs:
        @pl.when(exists[(dz, dy)])
        def _(dz=dz, dy=dy):
            pl.semaphore_signal(
                barrier, inc=1, device_id={"depth": di + dz, "lat": li + dy},
                device_id_type=pl.DeviceIdType.MESH,
            )

    def fill_layer(z, c):
        for hf in range(nh):
            lanes = slice(hf * 128, hf * 128 + 128)
            for comp in range(3):
                tiles[h + z, hf, pl.ds(hy * 8 + comp, ny, stride=8), :] = disp[comp, z, :, lanes]
                tiles[h + z, hf, pl.ds(hy * 8 + 4 + comp, ny, stride=8), :] = vel[comp, z, :, lanes]
            tiles[h + z, hf, pl.ds(hy * 8 + 3, ny, stride=8), :] = (mat[z, :, lanes] + 1).astype(f32)
            tiles[h + z, hf, pl.ds(hy * 8 + 7, ny, stride=8), :] = inv[z, :, lanes] * (-time_step)
        return c

    lax.fori_loop(0, nz, fill_layer, 0)

    @pl.when(is_bottom)
    def _():
        for hf in range(nh):
            lanes = slice(hf * 128, hf * 128 + 128)
            twice = 2.0 * mask[:, lanes].astype(f32)
            for s in range(steps):
                for comp in range(3):
                    pull[q_of[s], hf, pl.ds(hy * 8 + 4 + comp, ny, stride=8), :] = (
                        imp_ref[comp] * (twice * inc[s, comp, :, lanes])
                    )

    pl.semaphore_wait(barrier, sum(jnp.where(here, 1, 0) for here in exists.values()))

    def landing(n, dz, dy):
        if dz == 0:
            return land_y.at[n, (1 + dy) // 2]
        if dy == 0:
            return land_z.at[n, (1 + dz) // 2]
        return land_c.at[n, (1 + dz) // 2 * 2 + (1 + dy) // 2]

    def span(shift, length, base, width, outward):
        if shift == 0:
            return pl.ds(base, length)
        if outward:
            return pl.ds(0, width) if shift > 0 else pl.ds(w - width, width)
        return pl.ds(base, width) if shift < 0 else pl.ds(base + length - width, width)

    def parts_of(n):
        fields = [(0, w, pl.ds(0, 4 if n == 0 else 3))]
        if w > 1 or n == 0:
            fields.append((1, w - 1 if w > 1 else w, pl.ds(4, 4 if n == 0 else 3)))
        return fields

    def pieces(n, dz, dy, waits=False):
        k, back = dirs.index((dz, dy)), dirs.index((-dz, -dy))
        copies = []
        for f, width, sub in parts_of(n):
            here = landing(n, dz, dy).at[
                span(dz, nz, 0, width, True), :, span(dy, ny, 0, width, True), sub, :
            ]
            there = landing(n, -dz, -dy).at[
                span(-dz, nz, 0, width, True), :, span(-dy, ny, 0, width, True), sub, :
            ]
            mine = grid5.at[
                span(dz, nz, h, width, False), :, span(dy, ny, hy, width, False), sub, :
            ]
            copies.append(
                pltpu.make_async_remote_copy(
                    src_ref=here if waits else mine,
                    dst_ref=here if waits else there,
                    send_sem=send_sem.at[n, k, f],
                    recv_sem=recv_sem.at[n, k if waits else back, f],
                    device_id={"depth": di + dz, "lat": li + dy},
                    device_id_type=pl.DeviceIdType.MESH,
                )
            )
        return copies

    def pull_copy(dy, waits=False):
        src = pl.ds((hy if dy < 0 else hy + ny - (w - 1)) * 8, (w - 1) * 8)
        dst = pl.ds((hy + ny if dy < 0 else hy - (w - 1)) * 8, (w - 1) * 8)
        side = (1 + dy) // 2
        return pltpu.make_async_remote_copy(
            src_ref=pull.at[pl.ds(0, len(wide)), :, src, :],
            dst_ref=pull.at[pl.ds(0, len(wide)), :, dst, :],
            send_sem=q_send.at[side],
            recv_sem=q_recv.at[side if waits else 1 - side],
            device_id={"depth": di, "lat": li + dy},
            device_id_type=pl.DeviceIdType.MESH,
        )

    pull_dirs = [dy for dy in (-1, 1) if w > 1 and (0, dy) in exists]

    def start_all(n):
        for dz, dy in sorted(dirs, key=lambda d: -abs(d[0]) - abs(d[1])):
            @pl.when(exists[(dz, dy)])
            def _(dz=dz, dy=dy):
                for copy in pieces(n, dz, dy):
                    copy.start()

    rows = lax.broadcasted_iota(jnp.int32, (8, nx), 0)
    columns = lax.broadcasted_iota(jnp.int32, (8, nx), 1)
    top3 = rows < 3
    mid3 = (rows >= 4) & (rows < 7)
    inner = (rows < 6) & (columns < nx - 1)
    keep_out = columns > 0

    def load_tile(z, y):
        return jnp.concatenate([tiles[z, hf, pl.ds(y * 8, 8), :] for hf in range(nh)], 1)

    def put_split(z, y, tile):
        beside = pltpu.roll(pltpu.roll(tile, 3, 0), nx - 1, 1)
        both = jnp.where(top3, tile, jnp.where(inner, beside, 0.0))
        high = both.astype(bf16).astype(f32)
        split[z, y] = jnp.concatenate([high, both - high], 0).astype(bf16)

    def receive(n, dz, dy):
        z0 = {-1: 0, 0: h, 1: h + nz}[dz]
        y0 = {-1: hy - w, 0: hy, 1: hy + ny}[dy]
        zn, yn = nz if dz == 0 else w, ny if dy == 0 else w
        ref = landing(n, dz, dy)

        if n == 0:
            @pl.when(jnp.logical_not(exists[(dz, dy)]))
            def _():
                def clear(z, c):
                    for y in range(yn):
                        for hf in range(nh):
                            tiles[z0 + z, hf, pl.ds((y0 + y) * 8, 8), :] = jnp.zeros((8, 128), f32)
                        split[z0 + z, y0 + y] = jnp.zeros((16, nx), bf16)
                    return c

                lax.fori_loop(0, zn, clear, 0)

        @pl.when(exists[(dz, dy)])
        def _():
            for copy in pieces(n, dz, dy, True):
                copy.wait_recv()
            far_y = {-1: 0, 0: -1, 1: w - 1}[dy]

            def body(z, c):
                far_z = (z == 0) if dz < 0 else (z == w - 1)
                for y in range(yn):
                    new = jnp.concatenate([ref[z, hf, y, :, :] for hf in range(nh)], 1)
                    low = rows < (4 if n == 0 else 3)
                    full = (low | (rows >= 4)) if n == 0 else (low | mid3)
                    if w == 1:
                        valid = full if n == 0 else low
                    elif y == far_y:
                        valid = low
                    elif dz == 0:
                        valid = full
                    else:
                        valid = low | (full & jnp.logical_not(far_z))
                    old = jnp.zeros((8, nx), f32) if n == 0 else load_tile(z0 + z, y0 + y)
                    new = jnp.where(valid, new, old)
                    for hf in range(nh):
                        tiles[z0 + z, hf, pl.ds((y0 + y) * 8, 8), :] = new[:, hf * 128 : hf * 128 + 128]
                    put_split(z0 + z, y0 + y, new)
                return c

            lax.fori_loop(0, zn, body, 0)

    def sent(n):
        for dz, dy in dirs:
            @pl.when(exists[(dz, dy)])
            def _(dz=dz, dy=dy):
                for copy in pieces(n, dz, dy):
                    copy.wait_send()

    wet = jnp.where(rows == 4, imp_ref[0], jnp.where(rows == 5, imp_ref[1], imp_ref[2]))
    wet = jnp.where(mid3 & is_bottom, wet, 0.0)

    def products(z, e, opening):
        ya, yb = hy - 1 - e, hy + ny - 1 + e
        matrix = big_s[...]
        prev_low = prev_high = None
        results = []
        for y in range(ya, yb + 1):
            values = jnp.concatenate(
                [split[z, y], split[z, y + 1], split[z + 1, y], split[z + 1, y + 1]], 0
            )
            values = jnp.concatenate([values, values], 0)
            product = jnp.dot(matrix, values, preferred_element_type=f32)
            dil = jnp.concatenate([moduli[0, z, hf, pl.ds(y, 1), :] for hf in range(nh)], 1)
            shr = jnp.concatenate([moduli[1, z, hf, pl.ds(y, 1), :] for hf in range(nh)], 1)
            g = dil * product[0:32] + shr * product[32:64]
            if y > ya:
                low = None if opening else (g[0:8] + prev_low) + carry[y]
                results.append((y, low, g[16:24] + prev_high))
            prev_low, prev_high = g[8:16], g[24:32]
        return results

    def keep(results):
        for y, low, high in results:
            if low is not None:
                held[y] = low
            carry[y] = high

    def update(z, e, s, closing):
        for y in range(hy - e, hy + ny + e):
            force = held[y]
            tile = load_tile(z, y)
            if closing:
                pulled = jnp.concatenate(
                    [pull[q_of[s], hf, pl.ds(y * 8, 8), :] for hf in range(nh)], 1
                )
                force = force + (wet * tile - pulled)
            side = pltpu.roll(pltpu.roll(force, 4, 0), 1, 1)
            mass = jnp.concatenate(
                [tiles[z, hf, pl.ds(y * 8 + 7, 1), :] for hf in range(nh)], 1
            )
            whole = force + jnp.where(keep_out, side, 0.0)
            moved = tile + jnp.where(mid3, mass * whole, 0.0)
            tile = moved + jnp.where(top3, time_step * pltpu.roll(moved, 4, 0), 0.0)
            for hf in range(nh):
                tiles[z, hf, pl.ds(y * 8, 8), :] = tile[:, hf * 128 : hf * 128 + 128]
            if s < steps - 1:
                put_split(z, y, tile)

    start_all(0)
    for dy in pull_dirs:
        @pl.when(exists[(0, dy)] & is_bottom)
        def _(dy=dy):
            pull_copy(dy).start()

    i32 = jnp.int32
    ri = lax.broadcasted_iota(i32, (32, 24), 0)
    rc = lax.broadcasted_iota(i32, (32, 24), 1)
    r8 = ri % 8
    left = (r8 % 4 < 3) & (rc == (ri // 8) * 6 + jnp.where(r8 < 3, r8 + 3, r8 - 4))
    left = jnp.where(left, 1.0, 0.0).astype(bf16)
    ci = lax.broadcasted_iota(i32, (24, 64), 0)
    cc = lax.broadcasted_iota(i32, (24, 64), 1)
    right = (cc % 8 < 6) & (ci == (cc // 16) * 6 + cc % 8)
    right = jnp.where(right, 1.0, 0.0).astype(bf16)
    blocks = []
    for m in range(2):
        whole = stiff[m]
        upper = whole.astype(bf16)
        lower = (whole - upper.astype(f32)).astype(bf16)
        parts = []
        for part in (upper, lower):
            picked = jnp.dot(left, part, preferred_element_type=f32).astype(bf16)
            parts.append(jnp.dot(picked, right, preferred_element_type=f32))
        blocks.append(jnp.concatenate(parts, 1))
    big_s[...] = jnp.concatenate(blocks, 0).astype(bf16)

    def split_layer(z, c):
        for y in range(ny):
            put_split(h + z, hy + y, load_tile(h + z, hy + y))
        return c

    lax.fori_loop(0, nz, split_layer, 0)

    own_chunks = [y0 for y0 in range(0, ext_y, 8) if hy <= y0 and y0 + 8 <= hy + ny]
    other_chunks = [y0 for y0 in range(0, ext_y, 8) if y0 not in own_chunks]

    def lookup(chunks):
        def body(z, c):
            for hf in range(nh):
                for y0 in chunks:
                    kind = tiles[z, hf, pl.ds(y0 * 8 + 3, 8, stride=8), :]
                    dil = jnp.zeros((8, 128), f32)
                    shr = jnp.zeros((8, 128), f32)
                    for m in range(nmat):
                        hit = kind == float(m + 1)
                        dil = jnp.where(hit, dil_tab[m], dil)
                        shr = jnp.where(hit, shr_tab[m], shr)
                    moduli[0, z, hf, pl.ds(y0, 8), :] = dil
                    moduli[1, z, hf, pl.ds(y0, 8), :] = shr
            return c

        return body

    lax.fori_loop(h, h + nz, lookup(own_chunks), 0)

    for s in range(steps):
        n, e = s // w, extra[s]
        if s % w == 0:
            if s > 0:
                start_all(n)
            for dz, dy in dirs:
                receive(n, dz, dy)
            sent(n)
            if s == 0:
                for dy in pull_dirs:
                    @pl.when(exists[(0, dy)] & is_bottom)
                    def _(dy=dy):
                        pull_copy(dy).wait_send()
                        pull_copy(dy, True).wait_recv()
                lax.fori_loop(0, h, lookup(own_chunks + other_chunks), 0)
                lax.fori_loop(h + nz, ext_z, lookup(own_chunks + other_chunks), 0)
                lax.fori_loop(h, h + nz, lookup(other_chunks), 0)
        start = jnp.where(di == 0, h, h - e)
        stop = jnp.where(is_bottom, h + nz - 1, h + nz - 1 + e)
        keep(products(start - 1, e, True))
        keep(products(start, e, False))

        def body(z, c, e=e, s=s):
            results = products(z, e, False)
            update(z - 1, e, s, False)
            keep(results)
            return c

        lax.fori_loop(start + 1, stop + 1, body, 0)
        update(stop, e, s, True)

    def give(z, c):
        for hf in range(nh):
            lanes = slice(hf * 128, hf * 128 + 128)
            for comp in range(3):
                out_d[comp, z, :, lanes] = tiles[h + z, hf, pl.ds(hy * 8 + comp, ny, stride=8), :]
                out_v[comp, z, :, lanes] = tiles[h + z, hf, pl.ds(hy * 8 + 4 + comp, ny, stride=8), :]
        return c

    lax.fori_loop(0, nz, give, 0)


def solution(mesh):
    depths, lats = mesh.shape["depth"], mesh.shape["lat"]

    def per_device(disp, vel, inv, mat, dil_tab, shr_tab, stiff, imp, mask, inc):
        _, nz, ny, nx = disp.shape
        steps = inc.shape[0]
        w = min(WIDTH, nz, ny, steps)
        nh = nx // 128
        groups = -(-steps // w)
        ext_z = nz + 2 * w
        ext_y = -(-(-(-w // 8) * 8 + ny + w) // 8) * 8
        ndirs = (3 if depths > 1 else 1) * (3 if lats > 1 else 1) - 1
        smem = pl.BlockSpec(memory_space=pltpu.SMEM)
        vmem = pl.BlockSpec(memory_space=pltpu.VMEM)
        shape = jax.ShapeDtypeStruct(disp.shape, f32)
        return pl.pallas_call(
            functools.partial(kernel, (nz, ny, nx, steps, depths, lats, w)),
            out_shape=(shape, shape),
            in_specs=[smem] * 3 + [vmem] * 7,
            out_specs=(vmem, vmem),
            scratch_shapes=[
                pltpu.VMEM((ext_z, nh, ext_y, 8, 128), f32),
                pltpu.VMEM((ext_z, ext_y, 16, nx), bf16),
                pltpu.VMEM((2, ext_z, nh, ext_y, 128), f32),
                pltpu.VMEM((ext_y, 8, nx), f32),
                pltpu.VMEM((ext_y, 8, nx), f32),
                pltpu.VMEM((steps, nh, ext_y * 8, 128), f32),
                pltpu.VMEM((groups, 2, nz, nh, w, 8, 128), f32),
                pltpu.VMEM((groups, 2, w, nh, ny, 8, 128), f32),
                pltpu.VMEM((groups, 4, w, nh, w, 8, 128), f32),
                pltpu.VMEM((64, 128), bf16),
                pltpu.SemaphoreType.DMA((groups, ndirs, 2)),
                pltpu.SemaphoreType.DMA((groups, ndirs, 2)),
                pltpu.SemaphoreType.DMA((2,)),
                pltpu.SemaphoreType.DMA((2,)),
            ],
            compiler_params=pltpu.CompilerParams(
                collective_id=0, has_side_effects=True, vmem_limit_bytes=56 * 1024 * 1024
            ),
        )(dil_tab, shr_tab, imp, disp, vel, inv, mat, stiff, mask, inc)

    field = P(None, "depth", "lat", None)
    node = P("depth", "lat", None)
    in_specs = (field, field, node, node, P(), P(), P(), P(), P("lat", None), P(None, None, "lat", None))
    return jax.shard_map(
        per_device, mesh=mesh, in_specs=in_specs, out_specs=(field, field), check_vma=False
    )
```

```python
import functools

import jax
import jax.numpy as jnp
from jax import lax
from jax.experimental import pallas as pl
from jax.experimental.pallas import tpu as pltpu
from jax.sharding import PartitionSpec as P

time_step = 0.1
WIDTH = 2
f32 = jnp.float32
bf16 = jnp.bfloat16


def kernel(
    cfg, dil_tab, shr_tab, imp_ref, disp, vel, inv, mat, stiff, mask, inc, out,
    grid5, split, moduli, carry, held, pull, land_y, land_z, land_c, big_s,
    send_sem, recv_sem, q_send, q_recv,
):
    nz, ny, nx, steps, depths, lats, w = cfg
    h = w
    nh = nx // 128
    hy = -(-h // 8) * 8
    ext_z = nz + 2 * h
    ext_y = grid5.shape[2]
    tiles = grid5.reshape(ext_z, nh, ext_y * 8, 128)
    nmat = dil_tab.shape[0]
    di = lax.axis_index("depth")
    li = lax.axis_index("lat")
    exists = {}
    for dz in (-1, 0, 1):
        for dy in (-1, 0, 1):
            if dz == 0 and dy == 0:
                continue
            if (dz != 0 and depths == 1) or (dy != 0 and lats == 1):
                continue
            exists[(dz, dy)] = (
                (di + dz >= 0) & (di + dz < depths) & (li + dy >= 0) & (li + dy < lats)
            )
    dirs = list(exists)
    is_bottom = di == depths - 1
    extra = [w - 1 - s % w for s in range(steps)]
    if steps % w:
        for s in range(steps - steps % w, steps):
            extra[s] = steps - 1 - s
    wide = [s for s in range(steps) if extra[s] > 0]
    order = wide + [s for s in range(steps) if extra[s] == 0]
    q_of = {s: i for i, s in enumerate(order)}

    pull[...] = jnp.zeros_like(pull)
    barrier = pltpu.get_barrier_semaphore()
    for dz, dy in dirs:
        @pl.when(exists[(dz, dy)])
        def _(dz=dz, dy=dy):
            pl.semaphore_signal(
                barrier, inc=1, device_id={"depth": di + dz, "lat": li + dy},
                device_id_type=pl.DeviceIdType.MESH,
            )

    def fill_layer(z, c):
        for hf in range(nh):
            lanes = slice(hf * 128, hf * 128 + 128)
            for comp in range(3):
                tiles[h + z, hf, pl.ds(hy * 8 + comp, ny, stride=8), :] = disp[comp, z, :, lanes]
                tiles[h + z, hf, pl.ds(hy * 8 + 4 + comp, ny, stride=8), :] = vel[comp, z, :, lanes]
            tiles[h + z, hf, pl.ds(hy * 8 + 3, ny, stride=8), :] = (mat[z, :, lanes] + 1).astype(f32)
            tiles[h + z, hf, pl.ds(hy * 8 + 7, ny, stride=8), :] = inv[z, :, lanes] * (-time_step)
        return c

    lax.fori_loop(0, nz, fill_layer, 0, unroll=2)

    @pl.when(is_bottom)
    def _():
        for hf in range(nh):
            lanes = slice(hf * 128, hf * 128 + 128)
            twice = 2.0 * mask[:, lanes].astype(f32)
            for s in range(steps):
                for comp in range(3):
                    pull[q_of[s], hf, pl.ds(hy * 8 + 4 + comp, ny, stride=8), :] = (
                        imp_ref[comp] * (twice * inc[s, comp, :, lanes])
                    )

    pl.semaphore_wait(barrier, sum(jnp.where(here, 1, 0) for here in exists.values()))

    def landing(n, dz, dy):
        if dz == 0:
            return land_y.at[n, (1 + dy) // 2]
        if dy == 0:
            return land_z.at[n, (1 + dz) // 2]
        return land_c.at[n, (1 + dz) // 2 * 2 + (1 + dy) // 2]

    def span(shift, length, base, width, outward):
        if shift == 0:
            return pl.ds(base, length)
        if outward:
            return pl.ds(0, width) if shift > 0 else pl.ds(w - width, width)
        return pl.ds(base, width) if shift < 0 else pl.ds(base + length - width, width)

    def parts_of(n):
        fields = [(0, w, pl.ds(0, 4 if n == 0 else 3))]
        if w > 1 or n == 0:
            fields.append((1, w - 1 if w > 1 else w, pl.ds(4, 4 if n == 0 else 3)))
        return fields

    def pieces(n, dz, dy, waits=False):
        k, back = dirs.index((dz, dy)), dirs.index((-dz, -dy))
        copies = []
        for f, width, sub in parts_of(n):
            here = landing(n, dz, dy).at[
                span(dz, nz, 0, width, True), :, span(dy, ny, 0, width, True), sub, :
            ]
            there = landing(n, -dz, -dy).at[
                span(-dz, nz, 0, width, True), :, span(-dy, ny, 0, width, True), sub, :
            ]
            mine = grid5.at[
                span(dz, nz, h, width, False), :, span(dy, ny, hy, width, False), sub, :
            ]
            copies.append(
                pltpu.make_async_remote_copy(
                    src_ref=here if waits else mine,
                    dst_ref=here if waits else there,
                    send_sem=send_sem.at[n, k, f],
                    recv_sem=recv_sem.at[n, k if waits else back, f],
                    device_id={"depth": di + dz, "lat": li + dy},
                    device_id_type=pl.DeviceIdType.MESH,
                )
            )
        return copies

    def pull_copy(dy, waits=False):
        src = pl.ds((hy if dy < 0 else hy + ny - (w - 1)) * 8, (w - 1) * 8)
        dst = pl.ds((hy + ny if dy < 0 else hy - (w - 1)) * 8, (w - 1) * 8)
        side = (1 + dy) // 2
        return pltpu.make_async_remote_copy(
            src_ref=pull.at[pl.ds(0, len(wide)), :, src, :],
            dst_ref=pull.at[pl.ds(0, len(wide)), :, dst, :],
            send_sem=q_send.at[side],
            recv_sem=q_recv.at[side if waits else 1 - side],
            device_id={"depth": di, "lat": li + dy},
            device_id_type=pl.DeviceIdType.MESH,
        )

    pull_dirs = [dy for dy in (-1, 1) if w > 1 and (0, dy) in exists]

    def start_all(n):
        for dz, dy in sorted(dirs, key=lambda d: -abs(d[0]) - abs(d[1])):
            @pl.when(exists[(dz, dy)])
            def _(dz=dz, dy=dy):
                for copy in pieces(n, dz, dy):
                    copy.start()

    rows = lax.broadcasted_iota(jnp.int32, (8, nx), 0)
    columns = lax.broadcasted_iota(jnp.int32, (8, nx), 1)
    top3 = rows < 3
    mid3 = (rows >= 4) & (rows < 7)
    inner = (rows < 6) & (columns < nx - 1)
    keep_out = columns > 0

    def load_tile(z, y):
        return jnp.concatenate([tiles[z, hf, pl.ds(y * 8, 8), :] for hf in range(nh)], 1)

    def put_split(z, y, tile):
        beside = pltpu.roll(pltpu.roll(tile, 3, 0), nx - 1, 1)
        both = jnp.where(top3, tile, jnp.where(inner, beside, 0.0))
        high = both.astype(bf16).astype(f32)
        split[z, y] = jnp.concatenate([high, both - high], 0).astype(bf16)

    def receive(n, dz, dy):
        z0 = {-1: 0, 0: h, 1: h + nz}[dz]
        y0 = {-1: hy - w, 0: hy, 1: hy + ny}[dy]
        zn, yn = nz if dz == 0 else w, ny if dy == 0 else w
        ref = landing(n, dz, dy)

        if n == 0:
            @pl.when(jnp.logical_not(exists[(dz, dy)]))
            def _():
                def clear(z, c):
                    for y in range(yn):
                        for hf in range(nh):
                            tiles[z0 + z, hf, pl.ds((y0 + y) * 8, 8), :] = jnp.zeros((8, 128), f32)
                        split[z0 + z, y0 + y] = jnp.zeros((16, nx), bf16)
                    return c

                lax.fori_loop(0, zn, clear, 0)

        @pl.when(exists[(dz, dy)])
        def _():
            for copy in pieces(n, dz, dy, True):
                copy.wait_recv()
            far_y = {-1: 0, 0: -1, 1: w - 1}[dy]

            def body(z, c):
                far_z = (z == 0) if dz < 0 else (z == w - 1)
                for y in range(yn):
                    new = jnp.concatenate([ref[z, hf, y, :, :] for hf in range(nh)], 1)
                    low = rows < (4 if n == 0 else 3)
                    full = (low | (rows >= 4)) if n == 0 else (low | mid3)
                    if w == 1:
                        valid = full if n == 0 else low
                    elif y == far_y:
                        valid = low
                    elif dz == 0:
                        valid = full
                    else:
                        valid = low | (full & jnp.logical_not(far_z))
                    old = jnp.zeros((8, nx), f32) if n == 0 else load_tile(z0 + z, y0 + y)
                    new = jnp.where(valid, new, old)
                    for hf in range(nh):
                        tiles[z0 + z, hf, pl.ds((y0 + y) * 8, 8), :] = new[:, hf * 128 : hf * 128 + 128]
                    put_split(z0 + z, y0 + y, new)
                return c

            lax.fori_loop(0, zn, body, 0, unroll=zn)

    def sent(n):
        for dz, dy in dirs:
            @pl.when(exists[(dz, dy)])
            def _(dz=dz, dy=dy):
                for copy in pieces(n, dz, dy):
                    copy.wait_send()

    wet = jnp.where(rows == 4, imp_ref[0], jnp.where(rows == 5, imp_ref[1], imp_ref[2]))
    wet = jnp.where(mid3 & is_bottom, wet, 0.0)

    def products(z, e, opening):
        ya, yb = hy - 1 - e, hy + ny - 1 + e
        matrix = big_s[...]
        prev_low = prev_high = None
        results = []
        for y in range(ya, yb + 1):
            values = jnp.concatenate(
                [split[z, y], split[z, y + 1], split[z + 1, y], split[z + 1, y + 1]], 0
            )
            values = jnp.concatenate([values, values], 0)
            product = jnp.dot(matrix, values, preferred_element_type=f32)
            dil = jnp.concatenate([moduli[0, z, hf, pl.ds(y, 1), :] for hf in range(nh)], 1)
            shr = jnp.concatenate([moduli[1, z, hf, pl.ds(y, 1), :] for hf in range(nh)], 1)
            g = dil * product[0:32] + shr * product[32:64]
            if y > ya:
                low = None if opening else (g[0:8] + prev_low) + carry[y]
                results.append((y, low, g[16:24] + prev_high))
            prev_low, prev_high = g[8:16], g[24:32]
        return results

    def keep(results):
        for y, low, high in results:
            if low is not None:
                held[y] = low
            carry[y] = high

    def update(z, e, s, closing):
        for y in range(hy - e, hy + ny + e):
            force = held[y]
            tile = load_tile(z, y)
            if closing:
                pulled = jnp.concatenate(
                    [pull[q_of[s], hf, pl.ds(y * 8, 8), :] for hf in range(nh)], 1
                )
                force = force + (wet * tile - pulled)
            side = pltpu.roll(pltpu.roll(force, 4, 0), 1, 1)
            mass = jnp.concatenate(
                [tiles[z, hf, pl.ds(y * 8 + 7, 1), :] for hf in range(nh)], 1
            )
            whole = force + jnp.where(keep_out, side, 0.0)
            moved = tile + jnp.where(mid3, mass * whole, 0.0)
            tile = moved + jnp.where(top3, time_step * pltpu.roll(moved, 4, 0), 0.0)
            for hf in range(nh):
                tiles[z, hf, pl.ds(y * 8, 8), :] = tile[:, hf * 128 : hf * 128 + 128]
            if s < steps - 1:
                put_split(z, y, tile)

    start_all(0)
    for dy in pull_dirs:
        @pl.when(exists[(0, dy)] & is_bottom)
        def _(dy=dy):
            pull_copy(dy).start()

    i32 = jnp.int32
    ri = lax.broadcasted_iota(i32, (32, 24), 0)
    rc = lax.broadcasted_iota(i32, (32, 24), 1)
    r8 = ri % 8
    left = (r8 % 4 < 3) & (rc == (ri // 8) * 6 + jnp.where(r8 < 3, r8 + 3, r8 - 4))
    left = jnp.where(left, 1.0, 0.0).astype(bf16)
    ci = lax.broadcasted_iota(i32, (24, 64), 0)
    cc = lax.broadcasted_iota(i32, (24, 64), 1)
    right = (cc % 8 < 6) & (ci == (cc // 16) * 6 + cc % 8)
    right = jnp.where(right, 1.0, 0.0).astype(bf16)
    blocks = []
    for m in range(2):
        whole = stiff[m]
        upper = whole.astype(bf16)
        lower = (whole - upper.astype(f32)).astype(bf16)
        parts = []
        for part in (upper, lower):
            picked = jnp.dot(left, part, preferred_element_type=f32).astype(bf16)
            parts.append(jnp.dot(picked, right, preferred_element_type=f32))
        blocks.append(jnp.concatenate(parts, 1))
    big_s[...] = jnp.concatenate(blocks, 0).astype(bf16)

    def split_layer(z, c):
        for y in range(ny):
            put_split(h + z, hy + y, load_tile(h + z, hy + y))
        return c

    lax.fori_loop(0, nz, split_layer, 0, unroll=2)

    own_chunks = [y0 for y0 in range(0, ext_y, 8) if hy <= y0 and y0 + 8 <= hy + ny]
    other_chunks = [y0 for y0 in range(0, ext_y, 8) if y0 not in own_chunks]

    def lookup(chunks):
        def body(z, c):
            for hf in range(nh):
                for y0 in chunks:
                    kind = tiles[z, hf, pl.ds(y0 * 8 + 3, 8, stride=8), :]
                    dil = jnp.zeros((8, 128), f32)
                    shr = jnp.zeros((8, 128), f32)
                    for m in range(nmat):
                        hit = kind == float(m + 1)
                        dil = jnp.where(hit, dil_tab[m], dil)
                        shr = jnp.where(hit, shr_tab[m], shr)
                    moduli[0, z, hf, pl.ds(y0, 8), :] = dil
                    moduli[1, z, hf, pl.ds(y0, 8), :] = shr
            return c

        return body

    lax.fori_loop(h, h + nz, lookup(own_chunks), 0, unroll=4)

    for s in range(steps):
        n, e = s // w, extra[s]
        if s % w == 0:
            if s > 0:
                start_all(n)
            for dz, dy in sorted(dirs, key=lambda d: (abs(d[0]) + abs(d[1]), abs(d[0]))):
                receive(n, dz, dy)
            sent(n)
            if s == 0:
                for dy in pull_dirs:
                    @pl.when(exists[(0, dy)] & is_bottom)
                    def _(dy=dy):
                        pull_copy(dy).wait_send()
                        pull_copy(dy, True).wait_recv()
                lax.fori_loop(0, h, lookup(own_chunks + other_chunks), 0)
                lax.fori_loop(h + nz, ext_z, lookup(own_chunks + other_chunks), 0)
                lax.fori_loop(h, h + nz, lookup(other_chunks), 0, unroll=2)
        start = jnp.where(di == 0, h, h - e)
        stop = jnp.where(is_bottom, h + nz - 1, h + nz - 1 + e)
        keep(products(start - 1, e, True))
        keep(products(start, e, False))

        def body(z, c, e=e, s=s):
            results = products(z, e, False)
            update(z - 1, e, s, False)
            keep(results)
            return c

        lax.fori_loop(start + 1, stop + 1, body, 0)
        update(stop, e, s, True)

    def give(z, c):
        for hf in range(nh):
            lanes = slice(hf * 128, hf * 128 + 128)
            for comp in range(3):
                out[0, comp, z, :, lanes] = tiles[h + z, hf, pl.ds(hy * 8 + comp, ny, stride=8), :]
                out[1, comp, z, :, lanes] = tiles[h + z, hf, pl.ds(hy * 8 + 4 + comp, ny, stride=8), :]
        return c

    lax.fori_loop(0, nz, give, 0, unroll=2)


def solution(mesh):
    depths, lats = mesh.shape["depth"], mesh.shape["lat"]

    def per_device(disp, vel, inv, mat, dil_tab, shr_tab, stiff, imp, mask, inc):
        _, nz, ny, nx = disp.shape
        steps = inc.shape[0]
        w = min(WIDTH, nz, ny, steps)
        nh = nx // 128
        groups = -(-steps // w)
        ext_z = nz + 2 * w
        ext_y = -(-(-(-w // 8) * 8 + ny + w) // 8) * 8
        ndirs = (3 if depths > 1 else 1) * (3 if lats > 1 else 1) - 1
        smem = pl.BlockSpec(memory_space=pltpu.SMEM)
        vmem = pl.BlockSpec(memory_space=pltpu.VMEM)
        shape = jax.ShapeDtypeStruct(disp.shape, f32)
        both = pl.pallas_call(
            functools.partial(kernel, (nz, ny, nx, steps, depths, lats, w)),
            out_shape=jax.ShapeDtypeStruct((2, *disp.shape), f32),
            in_specs=[smem] * 3 + [vmem] * 7,
            out_specs=vmem,
            scratch_shapes=[
                pltpu.VMEM((ext_z, nh, ext_y, 8, 128), f32),
                pltpu.VMEM((ext_z, ext_y, 16, nx), bf16),
                pltpu.VMEM((2, ext_z, nh, ext_y, 128), f32),
                pltpu.VMEM((ext_y, 8, nx), f32),
                pltpu.VMEM((ext_y, 8, nx), f32),
                pltpu.VMEM((steps, nh, ext_y * 8, 128), f32),
                pltpu.VMEM((groups, 2, nz, nh, w, 8, 128), f32),
                pltpu.VMEM((groups, 2, w, nh, ny, 8, 128), f32),
                pltpu.VMEM((groups, 4, w, nh, w, 8, 128), f32),
                pltpu.VMEM((64, 128), bf16),
                pltpu.SemaphoreType.DMA((groups, ndirs, 2)),
                pltpu.SemaphoreType.DMA((groups, ndirs, 2)),
                pltpu.SemaphoreType.DMA((2,)),
                pltpu.SemaphoreType.DMA((2,)),
            ],
            compiler_params=pltpu.CompilerParams(
                collective_id=0, has_side_effects=True, vmem_limit_bytes=56 * 1024 * 1024
            ),
        )(dil_tab, shr_tab, imp, disp, vel, inv, mat, stiff, mask, inc)
        return both[0], both[1]

    field = P(None, "depth", "lat", None)
    node = P("depth", "lat", None)
    in_specs = (field, field, node, node, P(), P(), P(), P(), P("lat", None), P(None, None, "lat", None))
    return jax.shard_map(
        per_device, mesh=mesh, in_specs=in_specs, out_specs=(field, field), check_vma=False
    )
```
